32 devices in a mesh: lon: 8 (over y, x, core), lev: 4 (over z).
Axes of the slice: x: 2, y: 2, z: 4, core: 2. Of those that a mesh axis runs over, the one named last changes fastest.
Arguments:
- field: float32 [72, 128, 128], P('lev', 'lon'), may hold values from -6 to 6
- ens: bfloat16 [80, 72, 128, 128], P(None, 'lev', 'lon'), may hold values from -2 to 2
- sdev: float32 [72, 128, 128], P('lev', 'lon'), may hold values from 0.5 to 2
- lon_taper: bfloat16 [17], replicated, may hold values from 0 to 0.079589844
- static_taper: bfloat16 [17], replicated, may hold values from 0 to 0.079589844
- loc_vert: bfloat16 [72, 72], P('lev'), may hold values from -0.75 to 0.75
- static_vert: bfloat16 [72, 72], P('lev'), may hold values from -0.75 to 0.75
- obs_block: int32 [8192], P('lon'), may hold values from -1 to 127, as said below
- obs_value: float32 [8192], P('lon'), may hold values from -6 to 6
- obs_rinv: float32 [8192], P('lon'), may hold values from 0.25 to 4
- obs_horiz: float32 [8192, 128], P('lon'), may hold values from -0.5 to 0.5
- obs_vert: float32 [8192, 72], P('lon', 'lev'), may hold values from -0.75 to 0.75
Outputs:
- increment: float32 [72, 128, 128], P('lev', 'lon')
- adjoint_field: float32 [72, 128, 128], P('lev', 'lon')
- obs_cost: float32 [], replicated
The draws below stay inside these ranges and needn't reach their ends.
Inputs may be any that keep to these rules, and one draw needn't show every extreme that they name: `obs_block`: each longitude sector's 1024 slots name only blocks within that sector's longitudes; live slots come first, in non-falling block order; at least half of a sector's slots are live, and some sector has all its slots live.
All inputs are finite; a program needn't handle non-finite values.
Results may differ from the reference program's by a relative error of at most 0.0041.
Values may be sent and summed in bfloat16 or wider, within the bound.
A program may use at most 128 MiB of HBM per device.

```python
import math
import jax
import jax.numpy as jnp
from jax import lax

ENS = 80
LEV = 72
LAT = 128
LON_DEV = 16
OBS_DEV = 1024
HALO = 8
NLON = 128
NOBS = 8192


def draw_obs_block(key, part):
    groups = NOBS // OBS_DEV
    per_group = LON_DEV // 8 * (LAT // 16)
    key_ids = jax.random.fold_in(key, 11)
    key_live = jax.random.fold_in(key, 23)
    local = jnp.sort(jax.random.randint(key_ids, (groups, OBS_DEV), 0, per_group), axis=1)
    counts = jax.random.randint(key_live, (groups, 1), OBS_DEV // 2, OBS_DEV + 1)
    counts = counts.at[0, 0].set(OBS_DEV)
    slots = jnp.arange(OBS_DEV)[None, :]
    base = jnp.arange(groups)[:, None] * per_group
    ids = jnp.where(slots < counts, local + base, -1)
    return ids.reshape(-1).astype(jnp.int32)


def steps_of(stream_key, dims, shards, least, high):
    level, own = 1.0, jax.random.fold_in(stream_key, 6)
    for position, blocks in shards:
        steps = jnp.exp(jax.random.uniform(jax.random.fold_in(own, position), (blocks,), jnp.float32, least / len(shards), high / len(shards)))
        level = level * jnp.repeat(steps, dims[position] // blocks).reshape([-1 if axis == position else 1 for axis in range(len(dims))])
    return level


def noise(rng, dims, spread, most, cuts=(), dtype=jnp.bfloat16):
    entries = spread * jax.random.normal(rng, dims, jnp.float32)
    if cuts:
        entries = entries * steps_of(rng, dims, cuts, -0.22, 0.18)
    return jnp.clip(entries, -most, most).astype(dtype)


def setup_inputs(seed: int = 0) -> dict:
    key_list = jax.random.split(jax.random.key(seed), 13)
    field = noise(key_list[0], (LEV, NLON, LAT), 1.0, 6.0, ((0, 4), (1, 8)), jnp.float32)
    ens = noise(key_list[1], (ENS, LEV, NLON, LAT), 0.3, 2.0, ((1, 4), (2, 8)))
    sdev = jnp.clip(jnp.exp(math.log(2.0) - 1.3862944 * jax.random.uniform(key_list[2], (LEV, NLON, LAT), jnp.float32) ** steps_of(key_list[2], (LEV, NLON, LAT), ((0, 4), (1, 8)), -0.2, 0.2)), 0.5, 2.0)
    lon_taper = jnp.clip(jax.random.uniform(key_list[3], (2 * HALO + 1,), jnp.float32, 0.0, 0.079589844), 0.0, 0.079589844).astype(jnp.bfloat16)
    static_taper = jnp.clip(jax.random.uniform(key_list[4], (2 * HALO + 1,), jnp.float32, 0.0, 0.079589844), 0.0, 0.079589844).astype(jnp.bfloat16)
    loc_vert = noise(key_list[5], (LEV, LEV), LEV ** -0.5, 0.75, ((0, 4),))
    static_vert = noise(key_list[6], (LEV, LEV), LEV ** -0.5, 0.75, ((0, 4),))
    obs_block = draw_obs_block(jax.random.fold_in(key_list[12], 71), 0)
    obs_value = noise(key_list[8], (NOBS,), 1.0, 6.0, ((0, 8),), jnp.float32)
    obs_rinv = jnp.clip(jnp.exp(math.log(4.0) - 2.7725887 * jax.random.uniform(key_list[9], (NOBS,), jnp.float32) ** steps_of(key_list[9], (NOBS,), ((0, 8),), -0.2, 0.2)), 0.25, 4.0)
    obs_horiz = noise(key_list[10], (NOBS, 128), 128 ** -0.5, 0.5, ((0, 8),), jnp.float32)
    obs_vert = noise(key_list[11], (NOBS, LEV), LEV ** -0.5, 0.75, ((0, 8), (1, 4)), jnp.float32)
    return dict(field=field, ens=ens, sdev=sdev, lon_taper=lon_taper, static_taper=static_taper, loc_vert=loc_vert, static_vert=static_vert, obs_block=obs_block, obs_value=obs_value, obs_rinv=obs_rinv, obs_horiz=obs_horiz, obs_vert=obs_vert)


ens_weight = 0.8
static_weight = 0.5


def localize(zfield, taper, vmatrix):
    width = taper.shape[0]
    half = width // 2
    total = jnp.zeros(zfield.shape, jnp.float32)
    for offset in range(width):
        total = total + taper[offset].astype(jnp.float32) * jnp.roll(zfield, half - offset, axis=1).astype(jnp.float32)
    smooth = total.astype(jnp.bfloat16)
    levels = smooth.shape[0]
    flat = smooth.reshape(levels, -1)
    return jnp.dot(vmatrix, flat, preferred_element_type=jnp.float32).reshape(zfield.shape)


def reference(field, ens, sdev, lon_taper, static_taper, loc_vert, static_vert, obs_block, obs_value, obs_rinv, obs_horiz, obs_vert):
    def member(total, pert):
        zpert = (pert.astype(jnp.float32) * field).astype(jnp.bfloat16)
        return total + pert.astype(jnp.float32) * localize(zpert, lon_taper, loc_vert), None

    ens_sum, _ = lax.scan(member, jnp.zeros(field.shape, jnp.float32), ens)
    spart = (sdev * field).astype(jnp.bfloat16)
    static_sum = localize(spart, static_taper, static_vert)
    increment = ens_weight * ens_sum + static_weight * sdev * static_sum
    nblk = (NLON // 8) * (LAT // 16)
    blocks = increment.reshape(LEV, NLON // 8, 8, LAT // 16, 16).transpose(0, 1, 3, 2, 4).reshape(LEV, nblk, 128)
    groups = NOBS // OBS_DEV
    ids = obs_block.reshape(groups, OBS_DEV)
    values = obs_value.reshape(groups, OBS_DEV)
    rinv = obs_rinv.reshape(groups, OBS_DEV)
    horiz = obs_horiz.reshape(groups, OBS_DEV, 128)
    vert = obs_vert.reshape(groups, OBS_DEV, LEV)

    def observe(carry, items):
        block_ids, value, weight, hpart, vpart = items
        live = block_ids >= 0
        safe = jnp.where(live, block_ids, 0).astype(jnp.int32)
        picked = jnp.take(blocks, safe, axis=1)
        hz = jnp.einsum('ljc,jc->lj', picked, hpart, precision=lax.Precision.HIGHEST)
        hx = jnp.einsum('jl,lj->j', vpart, hz, precision=lax.Precision.HIGHEST)
        miss = hx - value
        dep = jnp.where(live, weight * miss, 0.0)
        cost = 0.5 * jnp.sum(dep * miss)
        terms = (dep[:, None, None] * vpart[:, :, None]) * hpart[:, None, :]
        adj = jax.ops.segment_sum(terms, safe, num_segments=nblk)
        return (carry[0] + adj, carry[1] + cost), None

    init = (jnp.zeros((nblk, LEV, 128), jnp.float32), jnp.zeros((), jnp.float32))
    (adj_blocks, obs_cost), _ = lax.scan(observe, init, (ids, values, rinv, horiz, vert))
    adjoint_field = adj_blocks.transpose(1, 0, 2).reshape(LEV, NLON // 8, LAT // 16, 8, 16).transpose(0, 1, 3, 2, 4).reshape(LEV, NLON, LAT)
    return increment, adjoint_field, obs_cost
```

```python
import functools

import jax
import jax.numpy as jnp
from jax import lax
from jax.experimental import pallas as pl
from jax.experimental.pallas import tpu as pltpu
from jax.sharding import PartitionSpec as P

ens_weight = 0.8
static_weight = 0.5
MESH = pl.DeviceIdType.MESH
F32 = jnp.float32
BF16 = jnp.bfloat16


def band_rows(taper, columns, lanes):
    width = taper.shape[0]
    offsets = jnp.arange(lanes)[None, :] - jnp.arange(columns)[:, None]
    onehot = (offsets[:, :, None] == jnp.arange(width)[None, None, :]).astype(F32)
    return jnp.sum(onehot * taper.astype(F32)[None, None, :], axis=2).astype(BF16)


def vert_rows(matrix, columns, lanes):
    rows, width = matrix.shape
    wide = jnp.pad(matrix, ((0, 0), (0, lanes - width)))
    return jnp.broadcast_to(wide[:, None, :], (rows, columns, lanes)).reshape(rows * columns, lanes)


def main_kernel(
    dims,
    ens,
    field,
    sdev,
    spart,
    lrep,
    srep,
    bands,
    out,
    ebuf,
    zbuf,
    hsend,
    fbuf,
    zs,
    ssend,
    lg,
    w,
    ws,
    pick,
    tband,
    acc,
    accb,
    rbuf,
    own_sem,
    ens_send,
    ens_recv,
    halo_send,
    halo_recv,
    small_send,
    small_recv,
    back_send,
    back_recv,
):
    nlev, nlon, levs, cols, half, pairs = dims
    rows = levs * cols
    full = nlev * rows
    edge = nlev * levs * half
    wide = full + 2 * edge
    me = lax.axis_index("lev")
    lon = lax.axis_index("lon")
    right, left = lax.rem(lon + 1, nlon), lax.rem(lon + nlon - 1, nlon)
    peers = [lax.rem(me + off, nlev) for off in range(1, nlev)]
    sources = [lax.rem(me + nlev - off, nlev) for off in range(1, nlev)]

    def slot(rank):
        return pl.ds(pl.multiple_of(rank * rows, 16), rows)

    own_copy = pltpu.make_async_copy(
        ens.at[pl.ds(me * 2 * pairs, 2 * pairs)], ebuf.at[:, slot(me)], own_sem
    )
    own_copy.start()

    barrier = pltpu.get_barrier_semaphore()
    for peer in peers:
        pl.semaphore_signal(barrier, inc=1, device_id={"lev": peer}, device_id_type=MESH)
    for peer in (left, right):
        pl.semaphore_signal(barrier, inc=1, device_id={"lon": peer}, device_id_type=MESH)
    pl.semaphore_wait(barrier, nlev + 1)

    def small(which, off, peer, rank):
        src, dst = ((lrep, lg), (field, fbuf), (spart, zs))[which]
        return pltpu.make_async_remote_copy(
            src_ref=src,
            dst_ref=dst.at[slot(rank)],
            send_sem=small_send.at[which, off],
            recv_sem=small_recv.at[which, off],
            device_id={"lev": peer},
            device_id_type=MESH,
        )

    def ens_copy(off, peer, rank, c):
        return pltpu.make_async_remote_copy(
            src_ref=ens.at[pl.ds(peer * 2 * pairs + 2 * c, 2)],
            dst_ref=ebuf.at[pl.ds(2 * c, 2), slot(rank)],
            send_sem=ens_send.at[off, c],
            recv_sem=ens_recv.at[off, c],
            device_id={"lev": peer},
            device_id_type=MESH,
        )

    def halo_copy(side, c):
        return pltpu.make_async_remote_copy(
            src_ref=hsend.at[side, c],
            dst_ref=zbuf.at[c, pl.ds(full + side * edge, edge)],
            send_sem=halo_send.at[side, c],
            recv_sem=halo_recv.at[side, c],
            device_id={"lon": (right, left)[side]},
            device_id_type=MESH,
        )

    def static_halo(side):
        return pltpu.make_async_remote_copy(
            src_ref=ssend.at[side],
            dst_ref=zs.at[pl.ds(full + side * edge, edge)],
            send_sem=halo_send.at[side, pairs],
            recv_sem=halo_recv.at[side, pairs],
            device_id={"lon": (right, left)[side]},
            device_id_type=MESH,
        )

    def back_copy(off, peer):
        return pltpu.make_async_remote_copy(
            src_ref=accb.at[slot(peer)],
            dst_ref=rbuf.at[off],
            send_sem=back_send.at[off],
            recv_sem=back_recv.at[off],
            device_id={"lev": peer},
            device_id_type=MESH,
        )

    for which in range(3):
        for off, peer in enumerate(peers):
            small(which, off, peer, me).start()

    def send_chunk(c, carry):
        for off, peer in enumerate(peers):
            ens_copy(off, peer, me, c).start()
        return carry

    lax.fori_loop(0, pairs, send_chunk, 0)

    lg[slot(me)] = lrep[...]
    fbuf[slot(me)] = field[...]
    zs[slot(me)] = spart[...]
    acc[...] = jnp.zeros_like(acc)

    lanes = lrep.shape[1]
    col = lax.broadcasted_iota(jnp.int32, (lanes, wide), 1)
    row = lax.broadcasted_iota(jnp.int32, (lanes, wide), 0)
    inner = col < full
    low = col < full + edge
    tail = jnp.where(low, col - full, col - full - edge)
    level = jnp.where(inner, col // cols, tail // half)
    place = jnp.where(
        inner, half + col % cols, jnp.where(low, tail % half, half + cols + tail % half)
    )
    pick[...] = jnp.where(row == level, 1.0, 0.0).astype(BF16)
    spots = jnp.where(row == place, 1.0, 0.0).astype(BF16)
    tband[...] = jnp.dot(bands[...], spots, preferred_element_type=F32)

    step = 6 * cols if (levs % 6) == 0 else cols

    def expand(src, dst, which, q):
        at = pl.ds(pl.multiple_of(q * step, 16), step)
        spread = jnp.dot(src[at], pick[...], preferred_element_type=F32)
        band = tband[which * cols : (which + 1) * cols]
        product = spread.reshape(step // cols, cols, wide) * band[None]
        dst[at] = product.reshape(step, wide).astype(BF16)

    def expand_static(q, carry):
        expand(srep, ws, 1, q)
        return carry

    lax.fori_loop(0, rows // step, expand_static, 0)

    for which in (0,):
        for off, rank in enumerate(sources):
            small(which, off, peers[off], rank).wait_recv()

    def expand_loc(q, carry):
        expand(lg, w, 0, q)
        return carry

    lax.fori_loop(0, full // step, expand_loc, 0)

    for which in (1, 2):
        for off, rank in enumerate(sources):
            small(which, off, peers[off], rank).wait_recv()

    def edges(values):
        split = values.reshape(nlev * levs, cols, values.shape[1])
        to_right = split[:, cols - half :].reshape(edge, values.shape[1]).astype(BF16)
        to_left = split[:, :half].reshape(edge, values.shape[1]).astype(BF16)
        return to_right, to_left

    ssend[0], ssend[1] = edges(zs[:full].astype(F32))
    own_copy.wait()
    for side in range(2):
        static_halo(side).start()

    tile = full // 3 if full % 48 == 0 else full

    def chunk(c, carry):
        @pl.when(c < pairs)
        def _():
            for off, rank in enumerate(sources):
                ens_copy(off, peers[off], rank, c).wait_recv()
            for h in range(2):
                at = slice(h * 128, (h + 1) * 128)
                product = ebuf[2 * c + h].astype(F32) * fbuf[...]
                hsend[0, c, :, at], hsend[1, c, :, at] = edges(product)
                zbuf[c, :full, at] = product.astype(BF16)
            for side in range(2):
                halo_copy(side, c).start()

        @pl.when(c >= 1)
        def _():
            d = c - 1
            for side in range(2):
                halo_copy(side, d).wait_recv()

            def piece(q, inner_carry):
                at = pl.ds(pl.multiple_of(q * tile, 16), tile)
                zv = jnp.dot(w[at], zbuf[d], preferred_element_type=F32)
                acc[at] += (
                    ebuf[2 * d, at].astype(F32) * zv[:, :128]
                    + ebuf[2 * d + 1, at].astype(F32) * zv[:, 128:]
                )
                return inner_carry

            lax.fori_loop(0, full // tile, piece, 0)

        return carry

    lax.fori_loop(0, pairs + 1, chunk, 0)

    accb[...] = acc[...].astype(BF16)
    for side in range(2):
        static_halo(side).wait_recv()
    static = jnp.dot(ws[...], zs[...], preferred_element_type=F32)
    base = static_weight * sdev[...] * static
    out[...] = base
    for off, peer in enumerate(peers):
        back_copy(off, peer).start()
    total = acc[slot(me)]
    for off, peer in enumerate(peers):
        back_copy(off, peer).wait_recv()
        total = total + rbuf[off].astype(F32)
    out[...] = out[...] + ens_weight * total

    for which in range(3):
        for off, peer in enumerate(peers):
            small(which, off, peer, me).wait_send()
    for off, peer in enumerate(peers):
        back_copy(off, peer).wait_send()
    for side in range(2):
        static_halo(side).wait_send()

    def drain(c, carry):
        for off, peer in enumerate(peers):
            ens_copy(off, peer, me, c).wait_send()
        for side in range(2):
            halo_copy(side, c).wait_send()
        return carry

    lax.fori_loop(0, pairs, drain, 0)


def covariance(field, ens, sdev, lon_taper, static_taper, loc_vert, static_vert, nlev, nlon):
    members, levs, cols, lats = ens.shape
    half = lon_taper.shape[0] // 2
    pairs = members // nlev // 2
    rows = levs * cols
    full = nlev * rows
    edge = nlev * levs * half
    wide = full + 2 * edge
    flat_field = field.reshape(rows, lats)
    flat_sdev = sdev.reshape(rows, lats)
    spart = (flat_sdev * flat_field).astype(BF16)
    lrep = vert_rows(loc_vert, cols, 128)
    srep = vert_rows(static_vert, cols, 128)
    bands = jnp.concatenate([band_rows(lon_taper, cols, 128), band_rows(static_taper, cols, 128)])
    vmem = pl.BlockSpec(memory_space=pltpu.VMEM)
    dma = pltpu.SemaphoreType.DMA
    out = pl.pallas_call(
        functools.partial(main_kernel, (nlev, nlon, levs, cols, half, pairs)),
        out_shape=jax.ShapeDtypeStruct((rows, lats), F32),
        in_specs=[pl.BlockSpec(memory_space=pl.ANY)] + [vmem] * 6,
        out_specs=vmem,
        scratch_shapes=[
            pltpu.VMEM((2 * pairs, full, lats), BF16),
            pltpu.VMEM((pairs, wide, 2 * lats), BF16),
            pltpu.VMEM((2, pairs, edge, 2 * lats), BF16),
            pltpu.VMEM((full, lats), F32),
            pltpu.VMEM((wide, lats), BF16),
            pltpu.VMEM((2, edge, lats), BF16),
            pltpu.VMEM((full, 128), BF16),
            pltpu.VMEM((full, wide), BF16),
            pltpu.VMEM((rows, wide), BF16),
            pltpu.VMEM((128, wide), BF16),
            pltpu.VMEM((2 * cols, wide), F32),
            pltpu.VMEM((full, lats), F32),
            pltpu.VMEM((full, lats), BF16),
            pltpu.VMEM((nlev - 1, rows, lats), BF16),
            dma,
            dma((nlev - 1, pairs)),
            dma((nlev - 1, pairs)),
            dma((2, pairs + 1)),
            dma((2, pairs + 1)),
            dma((3, nlev - 1)),
            dma((3, nlev - 1)),
            dma((nlev - 1,)),
            dma((nlev - 1,)),
        ],
        compiler_params=pltpu.CompilerParams(
            collective_id=0, has_side_effects=True, vmem_limit_bytes=60 * 1024 * 1024
        ),
        name="covariance",
    )(ens.reshape(members, rows, lats), flat_field, flat_sdev, spart, lrep, srep, bands)
    return out.reshape(levs, cols, lats)


def depart_kernel(
    nlev, nlon, part, value, rinv, live, dep, cost, parts, costs, psend, precv, csend, crecv
):
    me = lax.axis_index("lev")
    lon = lax.axis_index("lon")
    levs = [lax.rem(me + off, nlev) for off in range(1, nlev)]
    lons = [lax.rem(lon + off, nlon) for off in range(1, nlon)]
    barrier = pltpu.get_barrier_semaphore()
    for peer in levs:
        pl.semaphore_signal(barrier, inc=1, device_id={"lev": peer}, device_id_type=MESH)
    for peer in lons:
        pl.semaphore_signal(barrier, inc=1, device_id={"lon": peer}, device_id_type=MESH)
    pl.semaphore_wait(barrier, nlev + nlon - 2)

    def part_copy(off, rank):
        return pltpu.make_async_remote_copy(
            src_ref=part,
            dst_ref=parts.at[rank],
            send_sem=psend.at[off],
            recv_sem=precv.at[off],
            device_id={"lev": levs[off]},
            device_id_type=MESH,
        )

    def cost_copy(off, rank):
        return pltpu.make_async_remote_copy(
            src_ref=costs.at[lon],
            dst_ref=costs.at[rank],
            send_sem=csend.at[off],
            recv_sem=crecv.at[off],
            device_id={"lon": lons[off]},
            device_id_type=MESH,
        )

    for off in range(nlev - 1):
        part_copy(off, me).start()
    parts[me] = part[...]
    for off in range(nlev - 1):
        part_copy(off, lax.rem(me + nlev - off - 1, nlev)).wait_recv()
    hx = parts[0]
    for rank in range(1, nlev):
        hx = hx + parts[rank]
    miss = hx - value[...]
    weighted = jnp.where(live[...] >= 0, rinv[...] * miss, 0.0)
    costs[lon] = jnp.sum(weighted * miss, axis=0, keepdims=True) * 0.5 + jnp.zeros((8, 128), F32)
    dep[...] = weighted
    for off in range(nlon - 1):
        cost_copy(off, lon).start()
    for off in range(nlon - 1):
        cost_copy(off, lax.rem(lon + nlon - off - 1, nlon)).wait_recv()
    total = costs[0]
    for rank in range(1, nlon):
        total = total + costs[rank]
    cost[...] = jnp.sum(total[:1], axis=1, keepdims=True)
    for off in range(nlev - 1):
        part_copy(off, me).wait_send()
    for off in range(nlon - 1):
        cost_copy(off, lon).wait_send()


def departures(part, value, rinv, ids, nlev, nlon):
    shape = (part.shape[0] // 128, 128)
    vmem = pl.BlockSpec(memory_space=pltpu.VMEM)
    dma = pltpu.SemaphoreType.DMA
    dep, cost = pl.pallas_call(
        functools.partial(depart_kernel, nlev, nlon),
        out_shape=(jax.ShapeDtypeStruct(shape, F32), jax.ShapeDtypeStruct((1, 1), F32)),
        in_specs=[vmem] * 4,
        out_specs=(vmem, vmem),
        scratch_shapes=[
            pltpu.VMEM((nlev,) + shape, F32),
            pltpu.VMEM((nlon, 8, 128), F32),
            dma((nlev - 1,)),
            dma((nlev - 1,)),
            dma((nlon - 1,)),
            dma((nlon - 1,)),
        ],
        compiler_params=pltpu.CompilerParams(collective_id=1, has_side_effects=True),
        name="departures",
    )(part.reshape(shape), value.reshape(shape), rinv.reshape(shape), ids.reshape(shape))
    return dep.reshape(-1), cost[0, 0]


def body(
    nlev,
    nlon,
    field,
    ens,
    sdev,
    lon_taper,
    static_taper,
    loc_vert,
    static_vert,
    obs_block,
    obs_value,
    obs_rinv,
    obs_horiz,
    obs_vert,
):
    members, lev_rows, lon_cols, lat_rows = ens.shape
    increment = covariance(
        field, ens, sdev, lon_taper, static_taper, loc_vert, static_vert, nlev, nlon
    )
    block_lon = lon_cols // 8
    block_lat = lat_rows // 16
    nblk = block_lon * block_lat
    slots = obs_block.shape[0]
    blocks = (
        increment.reshape(lev_rows, block_lon, 8, block_lat, 16)
        .transpose(0, 1, 3, 2, 4)
        .reshape(lev_rows * nblk, 128)
    )
    live = obs_block >= 0
    local_ids = obs_block - lax.axis_index("lon") * nblk
    safe = jnp.where(live, local_ids, 0)
    selector = ((jnp.arange(nblk)[:, None] == safe[None, :]) & live[None, :]).astype(F32)
    vert = obs_vert.T
    projected = jnp.dot(blocks, obs_horiz.T, precision=lax.Precision.HIGHEST).reshape(
        lev_rows, nblk, slots
    )
    picked = jnp.sum(projected * selector[None], axis=1)
    partial_value = jnp.sum(picked * vert, axis=0)
    dep, obs_cost = departures(partial_value, obs_value, obs_rinv, obs_block, nlev, nlon)
    weights = vert * dep[None, :]
    spread = (weights[:, None, :] * selector[None]).reshape(lev_rows * nblk, slots)
    adj_blocks = jnp.dot(spread, obs_horiz, precision=lax.Precision.HIGHEST)
    adjoint_field = (
        adj_blocks.reshape(lev_rows, block_lon, block_lat, 8, 16)
        .transpose(0, 1, 3, 2, 4)
        .reshape(lev_rows, lon_cols, lat_rows)
    )
    return (increment, adjoint_field, obs_cost)


def solution(mesh):
    return jax.shard_map(
        functools.partial(body, mesh.shape["lev"], mesh.shape["lon"]),
        mesh=mesh,
        in_specs=(
            P("lev", "lon", None),
            P(None, "lev", "lon", None),
            P("lev", "lon", None),
            P(),
            P(),
            P("lev", None),
            P("lev", None),
            P("lon"),
            P("lon"),
            P("lon"),
            P("lon", None),
            P("lon", "lev"),
        ),
        out_specs=(P("lev", "lon", None), P("lev", "lon", None), P()),
        check_vma=False,
    )
```

```python
import functools

import jax
import jax.numpy as jnp
from jax import lax
from jax.experimental import pallas as pl
from jax.experimental.pallas import tpu as pltpu
from jax.sharding import PartitionSpec as P

ens_weight = 0.8
static_weight = 0.5
MESH = pl.DeviceIdType.MESH
F32 = jnp.float32
BF16 = jnp.bfloat16


def split(values):
    high = values.astype(BF16)
    return high, (values - high.astype(F32)).astype(BF16)


def swap_groups(source, target, count, lats):
    group = lax.broadcasted_iota(jnp.int32, (count, lats), 1) // 16
    for by in range(8):
        rows = jnp.zeros((count, lats), F32)
        for s in range(8):
            line = source[pl.ds(s, count, stride=8)]
            shift = (16 * (s - by)) % lats
            moved = pltpu.roll(line, shift, 1) if shift else line
            rows = jnp.where(group == s, moved, rows)
        target[pl.ds(by, count, stride=8)] = rows


def main_kernel(
    dims,
    ens,
    field,
    sdev,
    taper,
    static_taper,
    loc,
    svert,
    ids,
    value,
    rinv,
    horiz,
    vert,
    out,
    adj,
    cost,
    ebuf,
    zbuf,
    hsend,
    fbuf,
    spart,
    zs,
    ssend,
    lpad,
    spad,
    lg,
    spread,
    w,
    ws,
    pick,
    tband,
    acc,
    accb,
    rbuf,
    hhigh,
    hlow,
    blocks,
    part,
    parts,
    costs,
    own_sem,
    ens_send,
    ens_recv,
    halo_send,
    halo_recv,
    small_send,
    small_recv,
    back_send,
    back_recv,
    part_send,
    part_recv,
    cost_send,
    cost_recv,
):
    nlev, nlon, levs, cols, half, pairs = dims
    rows = levs * cols
    full = nlev * rows
    edge = nlev * levs * half
    wide = full + 2 * edge
    me = lax.axis_index("lev")
    lon = lax.axis_index("lon")
    right, left = lax.rem(lon + 1, nlon), lax.rem(lon + nlon - 1, nlon)
    peers = [lax.rem(me + off, nlev) for off in range(1, nlev)]
    sources = [lax.rem(me + nlev - off, nlev) for off in range(1, nlev)]

    def slot(rank):
        return pl.ds(pl.multiple_of(rank * rows, 16), rows)

    own_copy = pltpu.make_async_copy(
        ens.at[pl.ds(me * 2 * pairs, 2 * pairs)], ebuf.at[:, slot(me)], own_sem
    )
    own_copy.start()
    width = loc.shape[1]
    for matrix, padded in ((loc, lpad), (svert, spad)):
        padded[...] = jnp.zeros_like(padded)
        padded[:levs, :width] = matrix[...]
    spart[...] = (sdev[...] * field[...]).astype(BF16)
    lons = [lax.rem(lon + off, nlon) for off in range(1, nlon)]

    barrier = pltpu.get_barrier_semaphore()
    for peer in peers:
        pl.semaphore_signal(barrier, inc=1, device_id={"lev": peer}, device_id_type=MESH)
    for peer in lons:
        pl.semaphore_signal(barrier, inc=1, device_id={"lon": peer}, device_id_type=MESH)
    pl.semaphore_wait(barrier, nlev + nlon - 2)

    def small(which, off, peer, rank):
        src, dst = ((lpad, lg), (field, fbuf), (spart, zs))[which]
        return pltpu.make_async_remote_copy(
            src_ref=src,
            dst_ref=dst.at[rank] if which == 0 else dst.at[slot(rank)],
            send_sem=small_send.at[which, off],
            recv_sem=small_recv.at[which, off],
            device_id={"lev": peer},
            device_id_type=MESH,
        )

    def ens_copy(off, peer, rank, c):
        return pltpu.make_async_remote_copy(
            src_ref=ens.at[pl.ds(peer * 2 * pairs + 2 * c, 2)],
            dst_ref=ebuf.at[pl.ds(2 * c, 2), slot(rank)],
            send_sem=ens_send.at[off, c],
            recv_sem=ens_recv.at[off, c],
            device_id={"lev": peer},
            device_id_type=MESH,
        )

    def halo_copy(side, c):
        return pltpu.make_async_remote_copy(
            src_ref=hsend.at[side, c],
            dst_ref=zbuf.at[c, pl.ds(full + side * edge, edge)],
            send_sem=halo_send.at[side, c],
            recv_sem=halo_recv.at[side, c],
            device_id={"lon": (right, left)[side]},
            device_id_type=MESH,
        )

    def static_halo(side):
        return pltpu.make_async_remote_copy(
            src_ref=ssend.at[side],
            dst_ref=zs.at[pl.ds(full + side * edge, edge)],
            send_sem=halo_send.at[side, pairs],
            recv_sem=halo_recv.at[side, pairs],
            device_id={"lon": (right, left)[side]},
            device_id_type=MESH,
        )

    def back_copy(off, peer):
        return pltpu.make_async_remote_copy(
            src_ref=accb.at[slot(peer)],
            dst_ref=rbuf.at[off],
            send_sem=back_send.at[off],
            recv_sem=back_recv.at[off],
            device_id={"lev": peer},
            device_id_type=MESH,
        )

    def part_copy(off, peer, rank):
        return pltpu.make_async_remote_copy(
            src_ref=part,
            dst_ref=parts.at[rank],
            send_sem=part_send.at[off],
            recv_sem=part_recv.at[off],
            device_id={"lev": peer},
            device_id_type=MESH,
        )

    def cost_copy(off, rank):
        return pltpu.make_async_remote_copy(
            src_ref=costs.at[lon],
            dst_ref=costs.at[rank],
            send_sem=cost_send.at[off],
            recv_sem=cost_recv.at[off],
            device_id={"lon": lons[off]},
            device_id_type=MESH,
        )

    for which in range(3):
        for off, peer in enumerate(peers):
            small(which, off, peer, me).start()

    def send_chunk(c, carry):
        for off, peer in enumerate(peers):
            ens_copy(off, peer, me, c).start()
        return carry

    lax.fori_loop(0, pairs, send_chunk, 0)

    lg[me] = lpad[...]
    fbuf[slot(me)] = field[...]
    zs[slot(me)] = spart[...]
    acc[...] = jnp.zeros_like(acc)

    lanes = lpad.shape[1]
    col = lax.broadcasted_iota(jnp.int32, (lanes, wide), 1)
    row = lax.broadcasted_iota(jnp.int32, (lanes, wide), 0)
    inner = col < full
    low = col < full + edge
    tail = jnp.where(low, col - full, col - full - edge)
    level = jnp.where(inner, col // cols, tail // half)
    place = jnp.where(
        inner, half + col % cols, jnp.where(low, tail % half, half + cols + tail % half)
    )
    pick[...] = jnp.where(row == level, 1.0, 0.0).astype(BF16)
    spot = place[:cols] - lax.broadcasted_iota(jnp.int32, (cols, wide), 0)
    for which, weights in enumerate((taper, static_taper)):
        tap = weights[...].astype(F32)
        band = jnp.zeros((cols, wide), F32)
        for d in range(tap.shape[1]):
            band = jnp.where(spot == d, tap[:, d : d + 1], band)
        tband[which * cols : (which + 1) * cols] = band

    padrows = lpad.shape[0]

    def expand(dst, which, rank, first):
        def one(q, carry):
            line = spread[pl.ds(rank * padrows + q, 1)]
            at = pl.ds(pl.multiple_of((first + q) * cols, 16), cols)
            dst[at] = (line * tband[which * cols : (which + 1) * cols]).astype(BF16)
            return carry

        lax.fori_loop(0, levs, one, 0)

    spread[:padrows] = jnp.dot(spad[...], pick[...], preferred_element_type=F32)
    expand(ws, 1, 0, 0)
    hhigh[...], hlow[...] = split(horiz[...])

    for off, rank in enumerate(sources):
        small(0, off, peers[off], rank).wait_recv()

    def expand_loc(rank, carry):
        spread[pl.ds(pl.multiple_of(rank * padrows, 8), padrows)] = jnp.dot(
            lg[rank], pick[...], preferred_element_type=F32
        )
        expand(w, 0, rank, rank * levs)
        return carry

    lax.fori_loop(0, nlev, expand_loc, 0)

    for which in (1, 2):
        for off, rank in enumerate(sources):
            small(which, off, peers[off], rank).wait_recv()

    def edges(values):
        lines = values.reshape(nlev * levs, cols, values.shape[1])
        to_right = lines[:, cols - half :].reshape(edge, values.shape[1]).astype(BF16)
        to_left = lines[:, :half].reshape(edge, values.shape[1]).astype(BF16)
        return to_right, to_left

    ssend[0], ssend[1] = edges(zs[:full].astype(F32))
    own_copy.wait()
    for side in range(2):
        static_halo(side).start()

    tile = full // 3 if full % 48 == 0 else full

    def chunk(c, carry):
        @pl.when(c < pairs)
        def _():
            for off, rank in enumerate(sources):
                ens_copy(off, peers[off], rank, c).wait_recv()
            for h in range(2):
                at = slice(h * 128, (h + 1) * 128)
                product = ebuf[2 * c + h].astype(F32) * fbuf[...]
                hsend[0, c, :, at], hsend[1, c, :, at] = edges(product)
                zbuf[c, :full, at] = product.astype(BF16)
            for side in range(2):
                halo_copy(side, c).start()

        @pl.when(c >= 1)
        def _():
            d = c - 1
            for side in range(2):
                halo_copy(side, d).wait_recv()

            def piece(q, inner_carry):
                at = pl.ds(pl.multiple_of(q * tile, 16), tile)
                zv = jnp.dot(w[at], zbuf[d], preferred_element_type=F32)
                acc[at] += (
                    ebuf[2 * d, at].astype(F32) * zv[:, :128]
                    + ebuf[2 * d + 1, at].astype(F32) * zv[:, 128:]
                )
                return inner_carry

            lax.fori_loop(0, full // tile, piece, 0)

        return carry

    lax.fori_loop(0, pairs + 1, chunk, 0)

    accb[...] = acc[...].astype(BF16)
    for side in range(2):
        static_halo(side).wait_recv()
    static = jnp.dot(ws[...], zs[...], preferred_element_type=F32)
    base = static_weight * sdev[...] * static
    out[...] = base
    for off, peer in enumerate(peers):
        back_copy(off, peer).start()
    total = acc[slot(me)]
    for off, peer in enumerate(peers):
        back_copy(off, peer).wait_recv()
        total = total + rbuf[off].astype(F32)
    out[...] = out[...] + ens_weight * total

    count = rows // 8
    lats = out.shape[1]
    nblk = rows // levs
    slots = ids.shape[1]
    contract = (((1,), (1,)), ((), ()))
    local_ids = ids[...] - lon * nblk
    block = lax.broadcasted_iota(jnp.int32, (nblk, slots), 0)
    chosen = (block == local_ids) & (ids[...] >= 0)
    selector = jnp.where(chosen, 1.0, 0.0)
    swap_groups(out, blocks, count, lats)
    high, low_part = split(blocks[...])
    projected = lax.dot_general(high, hhigh[...], contract, preferred_element_type=F32)
    projected += lax.dot_general(low_part, hhigh[...], contract, preferred_element_type=F32)
    projected += lax.dot_general(high, hlow[...], contract, preferred_element_type=F32)
    picked = jnp.sum(projected.reshape(levs, nblk, slots) * selector[None], axis=1)
    mine = jnp.sum(picked * vert[...], axis=0, keepdims=True)
    part[...] = mine
    parts[me] = mine
    for off, peer in enumerate(peers):
        part_copy(off, peer, me).start()
    for off, rank in enumerate(sources):
        part_copy(off, peers[off], rank).wait_recv()
    hx = parts[0]
    for rank in range(1, nlev):
        hx = hx + parts[rank]
    miss = hx - value[...]
    dep = jnp.where(ids[...] >= 0, rinv[...] * miss, 0.0)
    terms = 0.5 * dep * miss
    folded = terms[:, :128]
    for q in range(1, slots // 128):
        folded = folded + terms[:, q * 128 : (q + 1) * 128]
    costs[lon] = folded
    weighted = vert[...] * dep
    spread_obs = (weighted[:, None, :] * selector[None]).reshape(rows, slots)
    high, low_part = split(spread_obs)
    for off in range(nlon - 1):
        cost_copy(off, lon).start()
    sums = jnp.dot(high, hhigh[...], preferred_element_type=F32)
    sums += jnp.dot(low_part, hhigh[...], preferred_element_type=F32)
    sums += jnp.dot(high, hlow[...], preferred_element_type=F32)
    blocks[...] = sums
    swap_groups(blocks, adj, count, lats)
    for off in range(nlon - 1):
        cost_copy(off, lax.rem(lon + nlon - off - 1, nlon)).wait_recv()
    total_cost = costs[0]
    for rank in range(1, nlon):
        total_cost = total_cost + costs[rank]
    cost[...] = jnp.sum(total_cost, axis=1, keepdims=True)
    for off, peer in enumerate(peers):
        part_copy(off, peer, me).wait_send()
    for off in range(nlon - 1):
        cost_copy(off, lon).wait_send()

    for which in range(3):
        for off, peer in enumerate(peers):
            small(which, off, peer, me).wait_send()
    for off, peer in enumerate(peers):
        back_copy(off, peer).wait_send()
    for side in range(2):
        static_halo(side).wait_send()

    def drain(c, carry):
        for off, peer in enumerate(peers):
            ens_copy(off, peer, me, c).wait_send()
        for side in range(2):
            halo_copy(side, c).wait_send()
        return carry

    lax.fori_loop(0, pairs, drain, 0)


def body(
    nlev,
    nlon,
    field,
    ens,
    sdev,
    lon_taper,
    static_taper,
    loc_vert,
    static_vert,
    obs_block,
    obs_value,
    obs_rinv,
    obs_horiz,
    obs_vert,
):
    members, levs, cols, lats = ens.shape
    half = lon_taper.shape[0] // 2
    pairs = members // nlev // 2
    rows = levs * cols
    full = nlev * rows
    edge = nlev * levs * half
    wide = full + 2 * edge
    slots = obs_block.shape[0]
    padrows = -(-levs // 16) * 16
    vmem = pl.BlockSpec(memory_space=pltpu.VMEM)
    dma = pltpu.SemaphoreType.DMA
    increment, adjoint_field, obs_cost = pl.pallas_call(
        functools.partial(main_kernel, (nlev, nlon, levs, cols, half, pairs)),
        out_shape=(
            jax.ShapeDtypeStruct((rows, lats), F32),
            jax.ShapeDtypeStruct((rows, lats), F32),
            jax.ShapeDtypeStruct((1, 1), F32),
        ),
        in_specs=[pl.BlockSpec(memory_space=pl.ANY)] + [vmem] * 11,
        out_specs=(vmem, vmem, vmem),
        scratch_shapes=[
            pltpu.VMEM((2 * pairs, full, lats), BF16),
            pltpu.VMEM((pairs, wide, 2 * lats), BF16),
            pltpu.VMEM((2, pairs, edge, 2 * lats), BF16),
            pltpu.VMEM((full, lats), F32),
            pltpu.VMEM((rows, lats), BF16),
            pltpu.VMEM((wide, lats), BF16),
            pltpu.VMEM((2, edge, lats), BF16),
            pltpu.VMEM((padrows, 128), BF16),
            pltpu.VMEM((padrows, 128), BF16),
            pltpu.VMEM((nlev, padrows, 128), BF16),
            pltpu.VMEM((nlev * padrows, wide), F32),
            pltpu.VMEM((full, wide), BF16),
            pltpu.VMEM((rows, wide), BF16),
            pltpu.VMEM((128, wide), BF16),
            pltpu.VMEM((2 * cols, wide), F32),
            pltpu.VMEM((full, lats), F32),
            pltpu.VMEM((full, lats), BF16),
            pltpu.VMEM((nlev - 1, rows, lats), BF16),
            pltpu.VMEM((slots, lats), BF16),
            pltpu.VMEM((slots, lats), BF16),
            pltpu.VMEM((rows, lats), F32),
            pltpu.VMEM((1, slots), F32),
            pltpu.VMEM((nlev, 1, slots), F32),
            pltpu.VMEM((nlon, 1, 128), F32),
            dma,
            dma((nlev - 1, pairs)),
            dma((nlev - 1, pairs)),
            dma((2, pairs + 1)),
            dma((2, pairs + 1)),
            dma((3, nlev - 1)),
            dma((3, nlev - 1)),
            dma((nlev - 1,)),
            dma((nlev - 1,)),
            dma((nlev - 1,)),
            dma((nlev - 1,)),
            dma((nlon - 1,)),
            dma((nlon - 1,)),
        ],
        compiler_params=pltpu.CompilerParams(
            collective_id=0, has_side_effects=True, vmem_limit_bytes=60 * 1024 * 1024
        ),
        name="covariance",
    )(
        ens.reshape(members, rows, lats),
        field.reshape(rows, lats),
        sdev.reshape(rows, lats),
        lon_taper.reshape(1, -1),
        static_taper.reshape(1, -1),
        loc_vert,
        static_vert,
        obs_block.reshape(1, slots),
        obs_value.reshape(1, slots),
        obs_rinv.reshape(1, slots),
        obs_horiz,
        obs_vert.T,
    )
    shape = (levs, cols, lats)
    return (increment.reshape(shape), adjoint_field.reshape(shape), obs_cost[0, 0])


def solution(mesh):
    return jax.shard_map(
        functools.partial(body, mesh.shape["lev"], mesh.shape["lon"]),
        mesh=mesh,
        in_specs=(
            P("lev", "lon", None),
            P(None, "lev", "lon", None),
            P("lev", "lon", None),
            P(),
            P(),
            P("lev", None),
            P("lev", None),
            P("lon"),
            P("lon"),
            P("lon"),
            P("lon", None),
            P("lon", "lev"),
        ),
        out_specs=(P("lev", "lon", None), P("lev", "lon", None), P()),
        check_vma=False,
    )
```

```python
import functools

import jax
import jax.numpy as jnp
from jax import lax
from jax.experimental import pallas as pl
from jax.experimental.pallas import tpu as pltpu
from jax.sharding import PartitionSpec as P

ens_weight = 0.8
static_weight = 0.5
MESH = pl.DeviceIdType.MESH
F32 = jnp.float32
BF16 = jnp.bfloat16


def split(values):
    high = values.astype(BF16)
    return high, (values - high.astype(F32)).astype(BF16)


def swap_groups(source, target, count, lats):
    group = lax.broadcasted_iota(jnp.int32, (count, lats), 1) // 16
    for by in range(8):
        rows = jnp.zeros((count, lats), F32)
        for s in range(8):
            line = source[pl.ds(s, count, stride=8)]
            shift = (16 * (s - by)) % lats
            moved = pltpu.roll(line, shift, 1) if shift else line
            rows = jnp.where(group == s, moved, rows)
        target[pl.ds(by, count, stride=8)] = rows


def main_kernel(
    dims,
    ens,
    field,
    sdev,
    taper,
    static_taper,
    loc,
    svert,
    ids,
    value,
    rinv,
    horiz,
    vert,
    out,
    adj,
    cost,
    ebuf,
    zbuf,
    hsend,
    fbuf,
    spart,
    zs,
    ssend,
    lpad,
    spad,
    lg,
    spread,
    w,
    ws,
    pick,
    tband,
    acc,
    accb,
    rbuf,
    hhigh,
    hlow,
    blocks,
    part,
    parts,
    costs,
    own_sem,
    ens_send,
    ens_recv,
    halo_send,
    halo_recv,
    small_send,
    small_recv,
    back_send,
    back_recv,
    part_send,
    part_recv,
    cost_send,
    cost_recv,
):
    nlev, nlon, levs, cols, half, pairs = dims
    rows = levs * cols
    full = nlev * rows
    edge = nlev * levs * half
    wide = full + 2 * edge
    me = lax.axis_index("lev")
    lon = lax.axis_index("lon")
    right, left = lax.rem(lon + 1, nlon), lax.rem(lon + nlon - 1, nlon)
    peers = [lax.rem(me + off, nlev) for off in range(1, nlev)]
    sources = [lax.rem(me + nlev - off, nlev) for off in range(1, nlev)]

    def slot(rank):
        return pl.ds(pl.multiple_of(rank * rows, 16), rows)

    own_copy = pltpu.make_async_copy(
        ens.at[pl.ds(me * 2 * pairs, 2 * pairs)], ebuf.at[:, slot(me)], own_sem
    )
    own_copy.start()
    width = loc.shape[1]
    for matrix, padded in ((loc, lpad), (svert, spad)):
        padded[...] = jnp.zeros_like(padded)
        padded[:levs, :width] = matrix[...]
    spart[...] = (sdev[...] * field[...]).astype(BF16)
    lons = [lax.rem(lon + off, nlon) for off in range(1, nlon)]

    barrier = pltpu.get_barrier_semaphore()
    for peer in peers:
        pl.semaphore_signal(barrier, inc=1, device_id={"lev": peer}, device_id_type=MESH)
    for peer in lons:
        pl.semaphore_signal(barrier, inc=1, device_id={"lon": peer}, device_id_type=MESH)
    pl.semaphore_wait(barrier, nlev + nlon - 2)

    def small(which, off, peer, rank):
        src, dst = ((lpad, lg), (field, fbuf), (spart, zs))[which]
        return pltpu.make_async_remote_copy(
            src_ref=src,
            dst_ref=dst.at[rank] if which == 0 else dst.at[slot(rank)],
            send_sem=small_send.at[which, off],
            recv_sem=small_recv.at[which, off],
            device_id={"lev": peer},
            device_id_type=MESH,
        )

    def ens_copy(off, peer, rank, c):
        return pltpu.make_async_remote_copy(
            src_ref=ens.at[peer * 2 * pairs + c],
            dst_ref=ebuf.at[c, slot(rank)],
            send_sem=ens_send.at[off, c],
            recv_sem=ens_recv.at[off, c],
            device_id={"lev": peer},
            device_id_type=MESH,
        )

    def halo_copy(side, c, h):
        at = pl.ds(h * 128, 128)
        return pltpu.make_async_remote_copy(
            src_ref=hsend.at[side, c, :, at],
            dst_ref=zbuf.at[c, pl.ds(full + side * edge, edge), at],
            send_sem=halo_send.at[side, 2 * c + h],
            recv_sem=halo_recv.at[side, 2 * c + h],
            device_id={"lon": (right, left)[side]},
            device_id_type=MESH,
        )

    def static_halo(side):
        return pltpu.make_async_remote_copy(
            src_ref=ssend.at[side],
            dst_ref=zs.at[pl.ds(full + side * edge, edge)],
            send_sem=halo_send.at[side, 2 * pairs],
            recv_sem=halo_recv.at[side, 2 * pairs],
            device_id={"lon": (right, left)[side]},
            device_id_type=MESH,
        )

    def back_copy(off, peer):
        return pltpu.make_async_remote_copy(
            src_ref=accb.at[slot(peer)],
            dst_ref=rbuf.at[off],
            send_sem=back_send.at[off],
            recv_sem=back_recv.at[off],
            device_id={"lev": peer},
            device_id_type=MESH,
        )

    def part_copy(off, peer, rank):
        return pltpu.make_async_remote_copy(
            src_ref=part,
            dst_ref=parts.at[rank],
            send_sem=part_send.at[off],
            recv_sem=part_recv.at[off],
            device_id={"lev": peer},
            device_id_type=MESH,
        )

    def cost_copy(off, rank):
        return pltpu.make_async_remote_copy(
            src_ref=costs.at[lon],
            dst_ref=costs.at[rank],
            send_sem=cost_send.at[off],
            recv_sem=cost_recv.at[off],
            device_id={"lon": lons[off]},
            device_id_type=MESH,
        )

    for which in range(2):
        for off, peer in enumerate(peers):
            small(which, off, peer, me).start()

    def send_chunk(c, carry):
        for off, peer in enumerate(peers):
            ens_copy(off, peer, me, c).start()
        return carry

    lax.fori_loop(0, 2 * pairs, send_chunk, 0)
    for off, peer in enumerate(peers):
        small(2, off, peer, me).start()

    lg[me] = lpad[...]
    fbuf[slot(me)] = field[...]
    zs[slot(me)] = spart[...]
    acc[...] = jnp.zeros_like(acc)

    lanes = lpad.shape[1]
    col = lax.broadcasted_iota(jnp.int32, (lanes, wide), 1)
    row = lax.broadcasted_iota(jnp.int32, (lanes, wide), 0)
    inner = col < full
    low = col < full + edge
    tail = jnp.where(low, col - full, col - full - edge)
    level = jnp.where(inner, col // cols, tail // half)
    place = jnp.where(
        inner, half + col % cols, jnp.where(low, tail % half, half + cols + tail % half)
    )
    pick[...] = jnp.where(row == level, 1.0, 0.0).astype(BF16)
    spot = place[:cols] - lax.broadcasted_iota(jnp.int32, (cols, wide), 0)
    for which, weights in enumerate((taper, static_taper)):
        tap = weights[...].astype(F32)
        band = jnp.zeros((cols, wide), F32)
        for d in range(tap.shape[1]):
            band = jnp.where(spot == d, tap[:, d : d + 1], band)
        tband[which * cols : (which + 1) * cols] = band

    padrows = lpad.shape[0]

    def expand(dst, which, rank, first):
        def one(q, carry):
            line = spread[pl.ds(rank * padrows + q, 1)]
            at = pl.ds(pl.multiple_of((first + q) * cols, 16), cols)
            dst[at] = (line * tband[which * cols : (which + 1) * cols]).astype(BF16)
            return carry

        lax.fori_loop(0, levs, one, 0)

    spread[:padrows] = jnp.dot(spad[...], pick[...], preferred_element_type=F32)
    expand(ws, 1, 0, 0)
    hhigh[...], hlow[...] = split(horiz[...])

    for off, rank in enumerate(sources):
        small(0, off, peers[off], rank).wait_recv()

    def expand_loc(rank, carry):
        spread[pl.ds(pl.multiple_of(rank * padrows, 8), padrows)] = jnp.dot(
            lg[rank], pick[...], preferred_element_type=F32
        )
        expand(w, 0, rank, rank * levs)
        return carry

    lax.fori_loop(0, nlev, expand_loc, 0)

    for off, rank in enumerate(sources):
        small(1, off, peers[off], rank).wait_recv()

    def edges(values):
        lines = values.reshape(nlev * levs, cols, values.shape[1])
        to_right = lines[:, cols - half :].reshape(edge, values.shape[1]).astype(BF16)
        to_left = lines[:, :half].reshape(edge, values.shape[1]).astype(BF16)
        return to_right, to_left

    own_copy.wait()

    tile = full // 3 if full % 48 == 0 else full

    def chunk(c, carry):
        @pl.when(c < pairs)
        def _():
            for h in range(2):
                for off, rank in enumerate(sources):
                    ens_copy(off, peers[off], rank, 2 * c + h).wait_recv()
                at = slice(h * 128, (h + 1) * 128)
                product = ebuf[2 * c + h].astype(F32) * fbuf[...]
                hsend[0, c, :, at], hsend[1, c, :, at] = edges(product)
                zbuf[c, :full, at] = product.astype(BF16)
                for side in range(2):
                    halo_copy(side, c, h).start()

        @pl.when(c == pairs)
        def _():
            for off, rank in enumerate(sources):
                small(2, off, peers[off], rank).wait_recv()
            ssend[0], ssend[1] = edges(zs[:full].astype(F32))
            for side in range(2):
                static_halo(side).start()

        @pl.when(c >= 1)
        def _():
            d = c - 1
            for h in range(2):
                for side in range(2):
                    halo_copy(side, d, h).wait_recv()

            def piece(q, inner_carry):
                at = pl.ds(pl.multiple_of(q * tile, 16), tile)
                zv = jnp.dot(w[at], zbuf[d], preferred_element_type=F32)
                acc[at] += (
                    ebuf[2 * d, at].astype(F32) * zv[:, :128]
                    + ebuf[2 * d + 1, at].astype(F32) * zv[:, 128:]
                )
                return inner_carry

            lax.fori_loop(0, full // tile, piece, 0)

        return carry

    lax.fori_loop(0, pairs + 1, chunk, 0)

    accb[...] = acc[...].astype(BF16)
    for side in range(2):
        static_halo(side).wait_recv()
    static = jnp.dot(ws[...], zs[...], preferred_element_type=F32)
    base = static_weight * sdev[...] * static
    out[...] = base
    for off, peer in enumerate(peers):
        back_copy(off, peer).start()
    total = acc[slot(me)]
    for off, peer in enumerate(peers):
        back_copy(off, peer).wait_recv()
        total = total + rbuf[off].astype(F32)
    out[...] = out[...] + ens_weight * total

    count = rows // 8
    lats = out.shape[1]
    nblk = rows // levs
    slots = ids.shape[1]
    contract = (((1,), (1,)), ((), ()))
    local_ids = ids[...] - lon * nblk
    block = lax.broadcasted_iota(jnp.int32, (nblk, slots), 0)
    chosen = (block == local_ids) & (ids[...] >= 0)
    selector = jnp.where(chosen, 1.0, 0.0)
    swap_groups(out, blocks, count, lats)
    high, low_part = split(blocks[...])
    projected = lax.dot_general(high, hhigh[...], contract, preferred_element_type=F32)
    projected += lax.dot_general(low_part, hhigh[...], contract, preferred_element_type=F32)
    projected += lax.dot_general(high, hlow[...], contract, preferred_element_type=F32)
    picked = jnp.sum(projected.reshape(levs, nblk, slots) * selector[None], axis=1)
    mine = jnp.sum(picked * vert[...], axis=0, keepdims=True)
    part[...] = mine
    parts[me] = mine
    for off, peer in enumerate(peers):
        part_copy(off, peer, me).start()
    for off, rank in enumerate(sources):
        part_copy(off, peers[off], rank).wait_recv()
    hx = parts[0]
    for rank in range(1, nlev):
        hx = hx + parts[rank]
    miss = hx - value[...]
    dep = jnp.where(ids[...] >= 0, rinv[...] * miss, 0.0)
    terms = 0.5 * dep * miss
    folded = terms[:, :128]
    for q in range(1, slots // 128):
        folded = folded + terms[:, q * 128 : (q + 1) * 128]
    costs[lon] = folded
    weighted = vert[...] * dep
    spread_obs = (weighted[:, None, :] * selector[None]).reshape(rows, slots)
    high, low_part = split(spread_obs)
    for off in range(nlon - 1):
        cost_copy(off, lon).start()
    sums = jnp.dot(high, hhigh[...], preferred_element_type=F32)
    sums += jnp.dot(low_part, hhigh[...], preferred_element_type=F32)
    sums += jnp.dot(high, hlow[...], preferred_element_type=F32)
    blocks[...] = sums
    swap_groups(blocks, adj, count, lats)
    for off in range(nlon - 1):
        cost_copy(off, lax.rem(lon + nlon - off - 1, nlon)).wait_recv()
    total_cost = costs[0]
    for rank in range(1, nlon):
        total_cost = total_cost + costs[rank]
    cost[...] = jnp.sum(total_cost, axis=1, keepdims=True)
    for off, peer in enumerate(peers):
        part_copy(off, peer, me).wait_send()
    for off in range(nlon - 1):
        cost_copy(off, lon).wait_send()

    for which in range(3):
        for off, peer in enumerate(peers):
            small(which, off, peer, me).wait_send()
    for off, peer in enumerate(peers):
        back_copy(off, peer).wait_send()
    for side in range(2):
        static_halo(side).wait_send()

    def drain(c, carry):
        for h in range(2):
            for off, peer in enumerate(peers):
                ens_copy(off, peer, me, 2 * c + h).wait_send()
            for side in range(2):
                halo_copy(side, c, h).wait_send()
        return carry

    lax.fori_loop(0, pairs, drain, 0)


def body(
    nlev,
    nlon,
    field,
    ens,
    sdev,
    lon_taper,
    static_taper,
    loc_vert,
    static_vert,
    obs_block,
    obs_value,
    obs_rinv,
    obs_horiz,
    obs_vert,
):
    members, levs, cols, lats = ens.shape
    half = lon_taper.shape[0] // 2
    pairs = members // nlev // 2
    rows = levs * cols
    full = nlev * rows
    edge = nlev * levs * half
    wide = full + 2 * edge
    slots = obs_block.shape[0]
    padrows = -(-levs // 16) * 16
    vmem = pl.BlockSpec(memory_space=pltpu.VMEM)
    dma = pltpu.SemaphoreType.DMA
    increment, adjoint_field, obs_cost = pl.pallas_call(
        functools.partial(main_kernel, (nlev, nlon, levs, cols, half, pairs)),
        out_shape=(
            jax.ShapeDtypeStruct((rows, lats), F32),
            jax.ShapeDtypeStruct((rows, lats), F32),
            jax.ShapeDtypeStruct((1, 1), F32),
        ),
        in_specs=[pl.BlockSpec(memory_space=pl.ANY)] + [vmem] * 11,
        out_specs=(vmem, vmem, vmem),
        scratch_shapes=[
            pltpu.VMEM((2 * pairs, full, lats), BF16),
            pltpu.VMEM((pairs, wide, 2 * lats), BF16),
            pltpu.VMEM((2, pairs, edge, 2 * lats), BF16),
            pltpu.VMEM((full, lats), F32),
            pltpu.VMEM((rows, lats), BF16),
            pltpu.VMEM((wide, lats), BF16),
            pltpu.VMEM((2, edge, lats), BF16),
            pltpu.VMEM((padrows, 128), BF16),
            pltpu.VMEM((padrows, 128), BF16),
            pltpu.VMEM((nlev, padrows, 128), BF16),
            pltpu.VMEM((nlev * padrows, wide), F32),
            pltpu.VMEM((full, wide), BF16),
            pltpu.VMEM((rows, wide), BF16),
            pltpu.VMEM((128, wide), BF16),
            pltpu.VMEM((2 * cols, wide), F32),
            pltpu.VMEM((full, lats), F32),
            pltpu.VMEM((full, lats), BF16),
            pltpu.VMEM((nlev - 1, rows, lats), BF16),
            pltpu.VMEM((slots, lats), BF16),
            pltpu.VMEM((slots, lats), BF16),
            pltpu.VMEM((rows, lats), F32),
            pltpu.VMEM((1, slots), F32),
            pltpu.VMEM((nlev, 1, slots), F32),
            pltpu.VMEM((nlon, 1, 128), F32),
            dma,
            dma((nlev - 1, 2 * pairs)),
            dma((nlev - 1, 2 * pairs)),
            dma((2, 2 * pairs + 1)),
            dma((2, 2 * pairs + 1)),
            dma((3, nlev - 1)),
            dma((3, nlev - 1)),
            dma((nlev - 1,)),
            dma((nlev - 1,)),
            dma((nlev - 1,)),
            dma((nlev - 1,)),
            dma((nlon - 1,)),
            dma((nlon - 1,)),
        ],
        compiler_params=pltpu.CompilerParams(
            collective_id=0, has_side_effects=True, vmem_limit_bytes=60 * 1024 * 1024
        ),
        name="covariance",
    )(
        ens.reshape(members, rows, lats),
        field.reshape(rows, lats),
        sdev.reshape(rows, lats),
        lon_taper.reshape(1, -1),
        static_taper.reshape(1, -1),
        loc_vert,
        static_vert,
        obs_block.reshape(1, slots),
        obs_value.reshape(1, slots),
        obs_rinv.reshape(1, slots),
        obs_horiz,
        obs_vert.T,
    )
    shape = (levs, cols, lats)
    return (increment.reshape(shape), adjoint_field.reshape(shape), obs_cost[0, 0])


def solution(mesh):
    return jax.shard_map(
        functools.partial(body, mesh.shape["lev"], mesh.shape["lon"]),
        mesh=mesh,
        in_specs=(
            P("lev", "lon", None),
            P(None, "lev", "lon", None),
            P("lev", "lon", None),
            P(),
            P(),
            P("lev", None),
            P("lev", None),
            P("lon"),
            P("lon"),
            P("lon"),
            P("lon", None),
            P("lon", "lev"),
        ),
        out_specs=(P("lev", "lon", None), P("lev", "lon", None), P()),
        check_vma=False,
    )
```
